32 devices in a mesh: seq: 8 (over z, x), mp: 4 (over y, core).
Axes of the slice: x: 2, y: 2, z: 4, core: 2. Of those that a mesh axis runs over, the one named last changes fastest.
Arguments:
- tokens: bfloat16 [256, 3584], P('mp'), may hold values from -6 to 6
- gain_attn: float32 [3584], replicated, may hold values from 0.25 to 1.75
- w_query: bfloat16 [3584, 3584], P(None, 'seq'), may hold values from -0.09375 to 0.09375
- query_bias: float32 [3584], P('seq'), may hold values from -3 to 3
- cache_keys: bfloat16 [4, 8192, 128], P(None, 'seq'), may hold values from -80 to 80
- cache_values: bfloat16 [4, 8192, 128], P(None, 'seq'), may hold values from -6 to 6
- w_out: bfloat16 [3584, 3584], P(None, 'seq'), may hold values from -0.09375 to 0.09375
- gain_ffn: float32 [3584], P('seq'), may hold values from 0.25 to 1.75
- w_gate: bfloat16 [3584, 18944], P('mp', 'seq'), may hold values from -0.09375 to 0.09375
- w_up: bfloat16 [3584, 18944], P('mp', 'seq'), may hold values from -0.09375 to 0.09375
- w_down: bfloat16 [18944, 3584], P('seq', 'mp'), may hold values from -0.0625 to 0.0625
Outputs:
- attended: bfloat16 [256, 3584], P('mp', 'seq')
- layer_out: bfloat16 [256, 3584], P('mp', 'seq')
The draws below stay inside these ranges and needn't reach their ends.
All inputs are finite; a program needn't handle non-finite values.
Results may differ from the reference program's by a relative error of at most 0.012.
The reference program's roundings to bfloat16 on the way (of `normed`, `queries`, `normed_ffn` and `activated`) count: a program that leaves them out, or rounds other values in their place, can miss the bound.
Values may be sent and summed in bfloat16 or wider, within the bound.
A program may use at most 64 MiB of HBM per device.

```python
import jax
import jax.numpy as jnp
from jax import lax

D = 3584
HEADS = 28
KV_HEADS = 4
HEAD = 128
FF = 18944
CTX_DEV = 1024
QUERIES = 256
CONTEXT = 8192
N_SEQ = 8


def draw_cache_keys(key, part):
    shape = (KV_HEADS, CONTEXT, HEAD)
    base_key, heavy_key, pick_key = jax.random.split(jax.random.fold_in(key, 17), 3)
    drawn = jnp.clip(2.7 * jax.random.normal(base_key, shape, jnp.float32), -16.0, 16.0)
    return drawn.astype(jnp.bfloat16)


def raised(values, own_key, source, target, blocks, factor):
    def block_of(axis_at):
        return (jnp.arange(values.shape[axis_at]) // (values.shape[axis_at] // blocks)).reshape((-1,) + (1,) * (values.ndim - 1 - axis_at))

    first = jax.random.permutation(own_key, blocks)[block_of(target)]
    far = (block_of(target) + blocks // 2) % blocks
    return jnp.where((block_of(source) == first) | (block_of(source) == far), factor * values, values)


def shard_levels(rng, extent, cuts, least, largest):
    loudness = 1.0
    for axis_at, blocks in cuts:
        draws = jax.random.uniform(jax.random.fold_in(jax.random.fold_in(rng, 6), axis_at), (blocks,), jnp.float32, least / len(cuts), largest / len(cuts))
        loudness = loudness * jnp.repeat(jnp.exp(draws), extent[axis_at] // blocks).reshape((-1,) + (1,) * (len(extent) - 1 - axis_at))
    return loudness


def centred(stream_key, extent, width, most, cuts=(), held_as=jnp.bfloat16):
    loudness = shard_levels(stream_key, extent, cuts, -0.22, 0.18) if cuts else 1.0
    values = jax.random.normal(stream_key, extent, jnp.float32) * width * loudness
    return jnp.minimum(jnp.maximum(values, -most), most).astype(held_as)


def heavy_noise(rng, dims, spread, most, cuts, heavy, kind=jnp.bfloat16):
    entries = spread * jax.random.normal(rng, dims, jnp.float32)
    if cuts:
        entries = entries * shard_levels(rng, dims, cuts, -0.22, 0.18)
    return jnp.clip(raised(entries, jax.random.fold_in(rng, 3), *heavy), -most, most).astype(kind)


def setup_inputs(seed: int = 0) -> dict:
    keys = jax.random.split(jax.random.key(seed), 12)
    return {
        "tokens": centred(keys[0], (QUERIES, D), 1.0, 6.0, ((0, 4),)),
        "gain_attn": jnp.clip(1.0 + 0.15 * jax.random.normal(keys[1], (D,), jnp.float32), 0.25, 1.75),
        "w_query": centred(keys[2], (D, D), D ** -0.5, 0.09375, ((1, 8),)),
        "query_bias": centred(keys[3], (D,), 0.5, 3.0, ((0, 8),), jnp.float32),
        "cache_keys": draw_cache_keys(jax.random.fold_in(keys[11], 71), 0),
        "cache_values": centred(keys[5], (KV_HEADS, CONTEXT, HEAD), 1.0, 6.0, ((1, 8),)),
        "w_out": centred(keys[6], (D, D), D ** -0.5, 0.09375, ((1, 8),)),
        "gain_ffn": jnp.clip(1.0 + 0.15 * jax.random.normal(keys[7], (D,), jnp.float32), 0.25, 1.75),
        "w_gate": centred(keys[8], (D, FF), D ** -0.5, 0.09375, ((0, 4), (1, 8))),
        "w_up": centred(keys[9], (D, FF), D ** -0.5, 0.09375, ((0, 4), (1, 8))),
        "w_down": heavy_noise(keys[10], (FF, D), FF ** -0.5, 0.0625, ((0, 8), (1, 4)), (0, 1, 8, 2.0)),
    }


eps = 1e-06

def expand(per_head):
    return jnp.repeat(per_head, HEAD, axis=1)

def block_attention(queries, block_keys, block_values):
    row_count = queries.shape[0]
    group_size = HEADS // KV_HEADS
    shaped = queries.reshape(row_count, KV_HEADS, group_size * HEAD)
    maxima = []
    sums = []
    outputs = []
    for head_group in range(KV_HEADS):
        block_query = shaped[:, head_group, :].reshape(row_count * group_size, HEAD)
        scores = jnp.einsum('rd,kd->rk', block_query.astype(jnp.float32), block_keys[head_group].astype(jnp.float32)) * HEAD ** (-0.5)
        highest = lax.optimization_barrier(jnp.max(scores, axis=1, keepdims=True))
        probs = jnp.exp(scores - highest)
        weight_sum = lax.optimization_barrier(jnp.sum(probs, axis=1))
        weighted = jnp.dot(probs.astype(jnp.bfloat16), block_values[head_group], preferred_element_type=jnp.float32)
        maxima.append(highest.reshape(row_count, group_size))
        sums.append(weight_sum.reshape(row_count, group_size))
        outputs.append(weighted.reshape(row_count, group_size * HEAD))
    return (jnp.concatenate(maxima, axis=1), jnp.concatenate(sums, axis=1), jnp.concatenate(outputs, axis=1))

def combine(first, second):
    highest = jnp.maximum(first[0], second[0])
    scale_one = jnp.exp(first[0] - highest)
    scale_two = jnp.exp(second[0] - highest)
    weight_sum = first[1] * scale_one + second[1] * scale_two
    weighted = first[2] * expand(scale_one) + second[2] * expand(scale_two)
    return (highest, weight_sum, weighted)

def reference(tokens, gain_attn, w_query, query_bias, cache_keys, cache_values, w_out, gain_ffn, w_gate, w_up, w_down):
    hidden_in = tokens.astype(jnp.float32)
    mean_sq = lax.optimization_barrier(jnp.mean(hidden_in * hidden_in, axis=1, keepdims=True))
    normed = (hidden_in * lax.rsqrt(mean_sq + eps) * gain_attn).astype(jnp.bfloat16)
    queries = (jnp.dot(normed, w_query, preferred_element_type=jnp.float32) + query_bias).astype(jnp.bfloat16)
    key_blocks = cache_keys.reshape(KV_HEADS, N_SEQ, CTX_DEV, HEAD).transpose(1, 0, 2, 3)
    value_blocks = cache_values.reshape(KV_HEADS, N_SEQ, CTX_DEV, HEAD).transpose(1, 0, 2, 3)
    start_state = block_attention(queries, key_blocks[0], value_blocks[0])

    def absorb(carried, blocks):
        return (combine(carried, block_attention(queries, blocks[0], blocks[1])), None)
    final_state, unused = lax.scan(absorb, start_state, (key_blocks[1:], value_blocks[1:]))
    attended = (final_state[2] / expand(final_state[1])).astype(jnp.bfloat16)
    residual = hidden_in + jnp.dot(attended, w_out, preferred_element_type=jnp.float32)
    mean_res = lax.optimization_barrier(jnp.mean(residual * residual, axis=1, keepdims=True))
    normed_ffn = (residual * lax.rsqrt(mean_res + eps) * gain_ffn).astype(jnp.bfloat16)
    gate_proj = jnp.dot(normed_ffn, w_gate, preferred_element_type=jnp.float32)
    up_proj = jnp.dot(normed_ffn, w_up, preferred_element_type=jnp.float32)
    activated = (jax.nn.silu(gate_proj) * up_proj).astype(jnp.bfloat16)
    ffn_sum = jnp.dot(activated, w_down, preferred_element_type=jnp.float32)
    layer_out = (residual + ffn_sum).astype(jnp.bfloat16)
    return (attended, layer_out)
```

```python
import functools

import jax
import jax.numpy as jnp
from jax import lax
from jax.experimental import pallas as pl
from jax.experimental.pallas import tpu as pltpu
from jax.sharding import PartitionSpec as P

D = 3584
HEADS = 28
KV_HEADS = 4
HEAD = 128
GROUP = HEADS // KV_HEADS
SUM_LANE = 64

eps = 1e-06
MESH = pl.DeviceIdType.MESH
VMEM = pltpu.VMEM


class SeqPlan:
    def __init__(self, n_seq, n_mp):
        self.count = n_seq

    def dest(self, s, m, i):
        to = lax.rem(s + i, self.count)
        return to, m, to

    def my_slot(self, s, m):
        return s

    def source(self, s, m, i):
        return i, m


class MpPlan:
    def __init__(self, n_seq, n_mp):
        self.count = n_mp

    def dest(self, s, m, i):
        to = lax.rem(m + i, self.count)
        return s, to, to

    def my_slot(self, s, m):
        return m

    def source(self, s, m, i):
        return s, i


class RowsPlan:
    def __init__(self, n_seq, n_mp):
        self.count, self.per = n_seq, n_seq // n_mp

    def dest(self, s, m, i):
        to = lax.rem(s + i, self.count)
        return to, s // self.per, to

    def my_slot(self, s, m):
        return m * self.per + lax.rem(s, self.per)

    def source(self, s, m, i):
        return m * self.per + i % self.per, i // self.per


class HomePlan:
    def __init__(self, n_seq, n_mp):
        self.count, self.per, self.n_mp = n_seq, n_seq // n_mp, n_mp

    def dest(self, s, m, i):
        to_m = lax.rem(m + i // self.per, self.n_mp)
        j = lax.rem(s + i, self.per)
        return m * self.per + j, to_m, to_m * self.per + j

    def my_slot(self, s, m):
        return s

    def source(self, s, m, i):
        return i, s // self.per


def exchange_kernel(plans, spread, *refs):
    k = len(plans)
    ins, outs, sems = refs[:k], refs[k : 2 * k], refs[2 * k :]
    s, m = lax.axis_index("seq"), lax.axis_index("mp")
    barrier = pltpu.get_barrier_semaphore()
    seen = []
    for plan in plans:
        if type(plan) in seen:
            continue
        seen.append(type(plan))
        for i in range(plan.count):
            fs, fm = plan.source(s, m, i)
            pl.semaphore_signal(barrier, inc=1, device_id=(fs, fm), device_id_type=MESH)
    done = []
    total = 0
    for plan in plans:
        if type(plan) not in done:
            done.append(type(plan))
            total += plan.count
    pl.semaphore_wait(barrier, total)
    steps = max(plan.count for plan in plans)
    waits = []
    for i in range(steps):
        for a in range(k):
            plan, src, dst = plans[a], ins[a], outs[a]
            if i >= plan.count:
                continue
            send, recv = sems[2 * a], sems[2 * a + 1]
            to_s, to_m, index = plan.dest(s, m, i)
            mine = plan.my_slot(s, m)
            block = src.at[index] if spread[a] else src
            here = jnp.logical_and(to_s == s, to_m == m)
            remote = pltpu.make_async_remote_copy(
                src_ref=block,
                dst_ref=dst.at[mine],
                send_sem=send.at[i],
                recv_sem=recv.at[mine],
                device_id=(to_s, to_m),
                device_id_type=MESH,
            )
            local = pltpu.make_async_copy(block, dst.at[mine], send.at[i])

            @pl.when(here)
            def _():
                local.start()

            @pl.when(jnp.logical_not(here))
            def _():
                remote.start()

            waits.append((here, local, remote))
    for a in range(k):
        plan, src, dst = plans[a], ins[a], outs[a]
        recv = sems[2 * a + 1]
        for i in range(plan.count):
            from_s, from_m = plan.source(s, m, i)
            here = jnp.logical_and(from_s == s, from_m == m)
            block = src.at[0] if spread[a] else src

            @pl.when(jnp.logical_not(here))
            def _():
                pltpu.make_async_remote_copy(
                    src_ref=block,
                    dst_ref=dst.at[i],
                    send_sem=recv.at[i],
                    recv_sem=recv.at[i],
                    device_id=(from_s, from_m),
                    device_id_type=MESH,
                ).wait_recv()

    for here, local, remote in waits:

        @pl.when(here)
        def _():
            local.wait()

        @pl.when(jnp.logical_not(here))
        def _():
            remote.wait_send()


def exchange(name, cid, *items):
    plans = [item[0] for item in items]
    arrays = [item[1] for item in items]
    spread = [item[2] for item in items]
    shapes = []
    sems = []
    for plan, array, one_each in items:
        block = array.shape[1:] if one_each else array.shape
        shapes.append(jax.ShapeDtypeStruct((plan.count,) + block, array.dtype))
        sems += [pltpu.SemaphoreType.DMA((plan.count,))] * 2
    return pl.pallas_call(
        functools.partial(exchange_kernel, plans, spread),
        out_shape=tuple(shapes),
        in_specs=[pl.BlockSpec(memory_space=VMEM)] * len(items),
        out_specs=tuple([pl.BlockSpec(memory_space=VMEM)] * len(items)),
        scratch_shapes=sems,
        compiler_params=pltpu.CompilerParams(collective_id=cid, has_side_effects=True),
        name=name,
    )(*arrays)


def attention_kernel(q_ref, k_ref, v_ref, out_ref, stat_ref):
    rows = q_ref.shape[0]
    q = q_ref[...]
    stacked = jnp.concatenate([q[:, h * HEAD : (h + 1) * HEAD] for h in range(GROUP)], axis=0)
    scores = lax.dot_general(
        stacked, k_ref[0], (((1,), (1,)), ((), ())), preferred_element_type=jnp.float32
    ) * HEAD ** (-0.5)
    highest = jnp.max(scores, axis=1, keepdims=True)
    probs = jnp.exp(scores - highest)
    sums = jnp.sum(probs, axis=1, keepdims=True)
    weighted = jnp.dot(probs.astype(jnp.bfloat16), v_ref[0], preferred_element_type=jnp.float32)
    lane = lax.broadcasted_iota(jnp.int32, (rows, 128), 1)
    base = pl.program_id(0) * GROUP
    stats = jnp.where(base == 0, jnp.zeros((rows, 128), jnp.float32), stat_ref[...])
    for h in range(GROUP):
        part = slice(h * rows, (h + 1) * rows)
        out_ref[:, h * HEAD : (h + 1) * HEAD] = weighted[part].astype(jnp.bfloat16)
        stats = jnp.where(lane == base + h, highest[part], stats)
        stats = jnp.where(lane == base + h + SUM_LANE, sums[part], stats)
    stat_ref[...] = stats


def attention(queries, keys, values):
    rows = queries.shape[0]
    context = keys.shape[1]
    width = GROUP * HEAD
    return pl.pallas_call(
        attention_kernel,
        grid=(KV_HEADS,),
        out_shape=(
            jax.ShapeDtypeStruct((rows, D), jnp.bfloat16),
            jax.ShapeDtypeStruct((rows, 128), jnp.float32),
        ),
        in_specs=[
            pl.BlockSpec((rows, width), lambda g: (0, g)),
            pl.BlockSpec((1, context, HEAD), lambda g: (g, 0, 0)),
            pl.BlockSpec((1, context, HEAD), lambda g: (g, 0, 0)),
        ],
        out_specs=(
            pl.BlockSpec((rows, width), lambda g: (0, g)),
            pl.BlockSpec((rows, 128), lambda g: (0, 0)),
        ),
        name="block_attention",
    )(queries, keys, values)


def joined(blocks):
    count, rows, width = blocks.shape
    return blocks.transpose(1, 0, 2).reshape(rows, count * width)


def body(
    n_seq,
    n_mp,
    tokens,
    gain_attn,
    w_query,
    query_bias,
    cache_keys,
    cache_values,
    w_out,
    gain_ffn,
    w_gate,
    w_up,
    w_down,
):
    seq, mp, to_rows, home = (kind(n_seq, n_mp) for kind in (SeqPlan, MpPlan, RowsPlan, HomePlan))
    per = n_seq // n_mp
    rows = tokens.shape[0]
    col_width = w_query.shape[1]
    offset = lax.axis_index("seq") * col_width
    hidden_in = tokens.astype(jnp.float32)
    mean_sq = jnp.mean(hidden_in * hidden_in, axis=1, keepdims=True)
    normed = (hidden_in * lax.rsqrt(mean_sq + eps) * gain_attn).astype(jnp.bfloat16)
    query_cols = (jnp.dot(normed, w_query, preferred_element_type=jnp.float32) + query_bias).astype(
        jnp.bfloat16
    )
    (query_blocks,) = exchange("queries", 1, (seq, query_cols, False))
    weighted, stats = attention(joined(query_blocks), cache_keys, cache_values)
    weighted = weighted.reshape(rows, n_seq, col_width).transpose(1, 0, 2)
    weighted, stats = exchange("merge", 2, (seq, weighted, True), (seq, stats, False))
    maxima, sums = stats[:, :, :HEADS], stats[:, :, SUM_LANE : SUM_LANE + HEADS]
    rescale = jnp.exp(maxima - jnp.max(maxima, axis=0, keepdims=True))
    totals = jnp.sum(sums * rescale, axis=0, keepdims=True)
    head_of = (offset + lax.broadcasted_iota(jnp.int32, (HEADS, col_width), 1)) // HEAD
    pick = (head_of == lax.broadcasted_iota(jnp.int32, (HEADS, col_width), 0)).astype(jnp.float32)
    factor = jnp.einsum(
        "jrh,hc->jrc", rescale / totals, pick, precision=lax.Precision.HIGHEST
    )
    attended = jnp.sum(weighted.astype(jnp.float32) * factor, axis=0).astype(jnp.bfloat16)
    (attended_blocks,) = exchange("attended", 3, (seq, attended, False))
    projected = jnp.dot(joined(attended_blocks), w_out, preferred_element_type=jnp.float32)
    residual = lax.dynamic_slice_in_dim(hidden_in, offset, col_width, 1) + projected
    square_part = jnp.sum(residual * residual, axis=1)[None, :]
    scaled = (residual * gain_ffn).astype(jnp.bfloat16)
    feature_blocks, square_parts = exchange(
        "residual", 4, (to_rows, scaled, False), (seq, square_part, False)
    )
    feature_block = (
        feature_blocks.reshape(n_mp, per, rows, col_width)
        .transpose(0, 2, 1, 3)
        .reshape(n_mp * rows, per * col_width)
    )
    gate_part = jnp.dot(feature_block, w_gate, preferred_element_type=jnp.float32)
    up_part = jnp.dot(feature_block, w_up, preferred_element_type=jnp.float32)
    hidden = w_gate.shape[1]
    gate_parts, up_parts = exchange(
        "gate_up",
        5,
        (mp, gate_part.astype(jnp.bfloat16).reshape(n_mp, rows, hidden), True),
        (mp, up_part.astype(jnp.bfloat16).reshape(n_mp, rows, hidden), True),
    )
    inverse = lax.rsqrt(jnp.sum(square_parts, axis=0)[0][:, None] / D + eps)
    gate_proj = jnp.sum(gate_parts.astype(jnp.float32), axis=0) * inverse
    up_proj = jnp.sum(up_parts.astype(jnp.float32), axis=0) * inverse
    own_activated = (jax.nn.silu(gate_proj) * up_proj).astype(jnp.bfloat16)
    (activated,) = exchange("activated", 6, (mp, own_activated, False))
    activated = activated.reshape(n_mp * rows, hidden)
    down_terms = jnp.dot(activated, w_down, preferred_element_type=jnp.float32).astype(jnp.bfloat16)
    down_blocks = (
        down_terms.reshape(n_mp, rows, per, col_width)
        .transpose(0, 2, 1, 3)
        .reshape(n_mp * per, rows, col_width)
    )
    (terms,) = exchange("down", 7, (home, down_blocks, True))
    layer_out = (residual + jnp.sum(terms.astype(jnp.float32), axis=0)).astype(jnp.bfloat16)
    return (attended, layer_out)


def solution(mesh):
    placed = (
        P("mp", None),
        P(),
        P(None, "seq"),
        P("seq"),
        P(None, "seq", None),
        P(None, "seq", None),
        P(None, "seq"),
        P("seq"),
        P("mp", "seq"),
        P("mp", "seq"),
        P("seq", "mp"),
    )
    return jax.shard_map(
        functools.partial(body, mesh.shape["seq"], mesh.shape["mp"]),
        mesh=mesh,
        in_specs=placed,
        out_specs=(P("mp", "seq"), P("mp", "seq")),
        check_vma=False,
    )
```

```python
import functools

import jax
import jax.numpy as jnp
from jax import lax
from jax.experimental import pallas as pl
from jax.experimental.pallas import tpu as pltpu
from jax.sharding import PartitionSpec as P

D = 3584
HEADS = 28
KV_HEADS = 4
HEAD = 128
GROUP = HEADS // KV_HEADS
SUM_LANE = 64
CHUNKS = 4

eps = 1e-06
MESH = pl.DeviceIdType.MESH
VMEM = pltpu.VMEM


class SeqPlan:
    def __init__(self, n_seq, n_mp):
        self.count = n_seq

    def dest(self, s, m, i):
        to = lax.rem(s + i, self.count)
        return to, m, to

    def my_slot(self, s, m):
        return s

    def source(self, s, m, i):
        return i, m


class RowsPlan:
    def __init__(self, n_seq, n_mp):
        self.count, self.per = n_seq, n_seq // n_mp

    def dest(self, s, m, i):
        to = lax.rem(s + i, self.count)
        return to, s // self.per, to

    def my_slot(self, s, m):
        return m * self.per + lax.rem(s, self.per)

    def source(self, s, m, i):
        return m * self.per + i % self.per, i // self.per


class HomePlan:
    def __init__(self, n_seq, n_mp):
        self.count, self.per, self.n_mp = n_seq, n_seq // n_mp, n_mp

    def dest(self, s, m, i):
        to_m = lax.rem(m + i // self.per, self.n_mp)
        j = lax.rem(s + i, self.per)
        return m * self.per + j, to_m, to_m * self.per + j

    def my_slot(self, s, m):
        return s

    def source(self, s, m, i):
        return i, s // self.per


def greet(plans, s, m):
    barrier = pltpu.get_barrier_semaphore()
    total = 0
    for plan in plans:
        for i in range(plan.count):
            pl.semaphore_signal(
                barrier, inc=1, device_id=plan.source(s, m, i), device_id_type=MESH
            )
        total += plan.count
    pl.semaphore_wait(barrier, total)


def push(src, dst, send, recv, to):
    return pltpu.make_async_remote_copy(
        src_ref=src,
        dst_ref=dst,
        send_sem=send,
        recv_sem=recv,
        device_id=to,
        device_id_type=MESH,
    )


class Flow:
    def __init__(self, plan, src, dst, spread, send, recv, s, m):
        self.plan, self.src, self.dst, self.spread = plan, src, dst, spread
        self.send, self.recv, self.s, self.m = send, recv, s, m
        self.started = []

    def start(self, i):
        to_s, to_m, index = self.plan.dest(self.s, self.m, i)
        mine = self.plan.my_slot(self.s, self.m)
        block = self.src.at[index] if self.spread else self.src
        here = jnp.logical_and(to_s == self.s, to_m == self.m)
        remote = push(block, self.dst.at[mine], self.send.at[i], self.recv.at[mine], (to_s, to_m))
        local = pltpu.make_async_copy(block, self.dst.at[mine], self.send.at[i])

        @pl.when(here)
        def _():
            local.start()

        @pl.when(jnp.logical_not(here))
        def _():
            remote.start()

        self.started.append((here, local, remote))

    def arrive(self):
        for i in range(self.plan.count):
            from_s, from_m = self.plan.source(self.s, self.m, i)
            block = self.src.at[0] if self.spread else self.src
            copy = push(block, self.dst.at[i], self.recv.at[i], self.recv.at[i], (from_s, from_m))

            @pl.when(jnp.logical_not(jnp.logical_and(from_s == self.s, from_m == self.m)))
            def _():
                copy.wait_recv()

        for here, local, remote in self.started:

            @pl.when(here)
            def _():
                local.wait()

    def left(self):
        for here, local, remote in self.started:

            @pl.when(jnp.logical_not(here))
            def _():
                remote.wait_send()


def exchange_kernel(plans, spread, *refs):
    k = len(plans)
    ins, outs, sems = refs[:k], refs[k : 2 * k], refs[2 * k :]
    s, m = lax.axis_index("seq"), lax.axis_index("mp")
    greet(list({type(plan): plan for plan in plans}.values()), s, m)
    flows = [
        Flow(plans[a], ins[a], outs[a], spread[a], sems[2 * a], sems[2 * a + 1], s, m)
        for a in range(k)
    ]
    for i in range(max(plan.count for plan in plans)):
        for flow in flows:
            if i < flow.plan.count:
                flow.start(i)
    for flow in flows:
        flow.arrive()
    for flow in flows:
        flow.left()


def exchange(name, cid, *items):
    plans = [item[0] for item in items]
    arrays = [item[1] for item in items]
    spread = [item[2] for item in items]
    shapes = []
    sems = []
    for plan, array, one_each in items:
        block = array.shape[1:] if one_each else array.shape
        shapes.append(jax.ShapeDtypeStruct((plan.count,) + block, array.dtype))
        sems += [pltpu.SemaphoreType.DMA((plan.count,))] * 2
    return pl.pallas_call(
        functools.partial(exchange_kernel, plans, spread),
        out_shape=tuple(shapes),
        in_specs=[pl.BlockSpec(memory_space=VMEM)] * len(items),
        out_specs=tuple([pl.BlockSpec(memory_space=VMEM)] * len(items)),
        scratch_shapes=sems,
        compiler_params=pltpu.CompilerParams(collective_id=cid, has_side_effects=True),
        name=name,
    )(*arrays)


def attention_kernel(q_ref, k_ref, v_ref, out_ref, stat_ref):
    rows = q_ref.shape[0]
    q = q_ref[...]
    stacked = jnp.concatenate([q[:, h * HEAD : (h + 1) * HEAD] for h in range(GROUP)], axis=0)
    scores = lax.dot_general(
        stacked, k_ref[0], (((1,), (1,)), ((), ())), preferred_element_type=jnp.float32
    ) * HEAD ** (-0.5)
    highest = jnp.max(scores, axis=1, keepdims=True)
    probs = jnp.exp(scores - highest)
    sums = jnp.sum(probs, axis=1, keepdims=True)
    weighted = jnp.dot(probs.astype(jnp.bfloat16), v_ref[0], preferred_element_type=jnp.float32)
    lane = lax.broadcasted_iota(jnp.int32, (rows, 128), 1)
    base = pl.program_id(0) * GROUP
    stats = jnp.where(base == 0, jnp.zeros((rows, 128), jnp.float32), stat_ref[...])
    for h in range(GROUP):
        part = slice(h * rows, (h + 1) * rows)
        out_ref[:, h * HEAD : (h + 1) * HEAD] = weighted[part].astype(jnp.bfloat16)
        stats = jnp.where(lane == base + h, highest[part], stats)
        stats = jnp.where(lane == base + h + SUM_LANE, sums[part], stats)
    stat_ref[...] = stats


def attention(queries, keys, values):
    rows = queries.shape[0]
    context = keys.shape[1]
    width = GROUP * HEAD
    return pl.pallas_call(
        attention_kernel,
        grid=(KV_HEADS,),
        out_shape=(
            jax.ShapeDtypeStruct((rows, D), jnp.bfloat16),
            jax.ShapeDtypeStruct((rows, 128), jnp.float32),
        ),
        in_specs=[
            pl.BlockSpec((rows, width), lambda g: (0, g)),
            pl.BlockSpec((1, context, HEAD), lambda g: (g, 0, 0)),
            pl.BlockSpec((1, context, HEAD), lambda g: (g, 0, 0)),
        ],
        out_specs=(
            pl.BlockSpec((rows, width), lambda g: (0, g)),
            pl.BlockSpec((rows, 128), lambda g: (0, 0)),
        ),
        name="block_attention",
    )(queries, keys, values)


def row_to_column(row):
    k = row.shape[1]
    across = lax.broadcasted_iota(jnp.int32, (k, k), 1)
    down = lax.broadcasted_iota(jnp.int32, (k, k), 0)
    return jnp.sum(jnp.where(across == down, row, 0.0), axis=1, keepdims=True)


def ffn_kernel(plans, bounds, *refs):
    seq, to_rows, home = plans
    scaled, square, residual, gate_hbm, up_hbm, down_hbm, out = refs[:7]
    refs = refs[7:]
    gate_w, up_w, down_w, blocks, squares, features, acc, down_out, terms = refs[:9]
    refs = refs[9:]
    w_sems, sems = refs[0], refs[1:7]
    c_sems = refs[7]
    chunk_refs = refs[8:]
    s, m = lax.axis_index("seq"), lax.axis_index("mp")
    core, y = lax.rem(m, 2), m // 2
    sibling = (s, y * 2 + (1 - core))
    across = (s, (1 - y) * 2 + core)
    rows, width = scaled.shape
    per, n_mp = to_rows.per, home.n_mp
    loads = [
        pltpu.make_async_copy(gate_hbm, gate_w, w_sems.at[0]),
        pltpu.make_async_copy(up_hbm, up_w, w_sems.at[1]),
        pltpu.make_async_copy(down_hbm, down_w, w_sems.at[2]),
    ]
    for load in loads:
        load.start()
    barrier = pltpu.get_barrier_semaphore()
    for peer in (sibling, across):
        pl.semaphore_signal(barrier, inc=1, device_id=peer, device_id_type=MESH)
    for plan in plans:
        for i in range(plan.count):
            pl.semaphore_signal(
                barrier, inc=1, device_id=plan.source(s, m, i), device_id_type=MESH
            )
    pl.semaphore_wait(barrier, 2 + sum(plan.count for plan in plans))
    main = Flow(to_rows, scaled, blocks, False, sems[0], sems[1], s, m)
    side = Flow(seq, square, squares, False, sems[2], sems[3], s, m)
    for i in range(to_rows.count):
        main.start(i)
    for i in range(seq.count):
        side.start(i)
    main.arrive()
    order = (1 - core, 3 - core, core, 2 + core)
    for p, t in enumerate(order):
        features[p * rows : (p + 1) * rows, :] = jnp.concatenate(
            [blocks[t * per + j] for j in range(per)], axis=1
        )
    loads[0].wait()
    loads[1].wait()

    chunks = []
    for c, (first, last) in enumerate(bounds):
        kept, s1_out, s1_in, s2_out, s2_in, act = chunk_refs[6 * c : 6 * c + 6]
        sem = lambda k, c=c: c_sems.at[c, k]
        chunks.append(
            dict(
                first=first, last=last, kept=kept, s1_out=s1_out, s1_in=s1_in,
                s2_out=s2_out, s2_in=s2_in, act=act,
                s1=push(s1_out, s1_in, sem(0), sem(1), sibling),
                s2=push(s2_out, s2_in, sem(2), sem(3), across),
                near=push(act.at[m], act.at[m], sem(4), sem(5), sibling),
                far=push(act.at[m], act.at[m], sem(6), sem(7), across),
                relay=push(act.at[across[1]], act.at[across[1]], sem(8), sem(9), sibling),
            )
        )

    def multiply(ch):
        for g, weight in enumerate((gate_w, up_w)):
            part = jnp.dot(
                features[...], weight[:, ch["first"] : ch["last"]],
                preferred_element_type=jnp.float32,
            )
            for p in range(2):
                ch["s1_out"][g, p] = part[p * rows : (p + 1) * rows].astype(jnp.bfloat16)
                ch["kept"][g, p] = part[(p + 2) * rows : (p + 3) * rows]
        ch["s1"].start()

    def pair_sum(ch):
        ch["s1"].wait_recv()
        for g in range(2):
            ch["s2_out"][g] = (
                ch["kept"][g, 1 - y] + ch["s1_in"][g, 1 - y].astype(jnp.float32)
            ).astype(jnp.bfloat16)
        ch["s2"].start()

    def activate(ch, inverse):
        ch["s2"].wait_recv()
        total = [
            (
                ch["kept"][g, y]
                + ch["s1_in"][g, y].astype(jnp.float32)
                + ch["s2_in"][g].astype(jnp.float32)
            )
            * inverse
            for g in range(2)
        ]
        gate, up = total
        ch["act"][m] = (gate / (1.0 + jnp.exp(-gate)) * up).astype(jnp.bfloat16)
        ch["far"].start()
        ch["near"].start()

    for c, ch in enumerate(chunks):
        multiply(ch)
        if c >= 1:
            pair_sum(chunks[c - 1])
    pair_sum(chunks[-1])
    side.arrive()
    inverse = row_to_column(lax.rsqrt(jnp.sum(squares[...], axis=0) / D + eps))
    for ch in chunks:
        activate(ch, inverse)
    loads[2].wait()
    for c, ch in enumerate(chunks):
        ch["far"].wait_recv()
        ch["relay"].start()
        ch["near"].wait_recv()
        ch["relay"].wait_recv()
        act = ch["act"][...].reshape(n_mp * rows, ch["last"] - ch["first"])
        part = jnp.dot(
            act, down_w[ch["first"] : ch["last"], :], preferred_element_type=jnp.float32
        )
        if c < len(chunks) - 1:
            acc[...] = part if c == 0 else acc[...] + part
        else:
            total = part if c == 0 else acc[...] + part
            for t in range(n_mp):
                for j in range(per):
                    down_out[t * per + j] = total[
                        t * rows : (t + 1) * rows, j * width : (j + 1) * width
                    ].astype(jnp.bfloat16)
    last = Flow(home, down_out, terms, True, sems[4], sems[5], s, m)
    for i in range(home.count):
        last.start(i)
    last.arrive()
    result = residual[...]
    for i in range(home.count):
        result = result + terms[i].astype(jnp.float32)
    out[...] = result.astype(jnp.bfloat16)
    main.left()
    side.left()
    last.left()
    for ch in chunks:
        for name in ("s1", "s2", "near", "far", "relay"):
            ch[name].wait_send()


def ffn(plans, scaled, square, residual, w_gate, w_up, w_down):
    seq, to_rows, home = plans
    rows, width = scaled.shape
    n_mp, n = home.n_mp, home.count
    hidden = w_gate.shape[1]
    step = max(128, -(-hidden // CHUNKS // 128) * 128)
    bounds = [(at, min(at + step, hidden)) for at in range(0, hidden, step)]
    bf16, f32 = jnp.bfloat16, jnp.float32
    scratch = [
        VMEM(w_gate.shape, bf16),
        VMEM(w_up.shape, bf16),
        VMEM(w_down.shape, bf16),
        VMEM((n, rows, width), bf16),
        VMEM((n, 1, rows), f32),
        VMEM((n_mp * rows, w_gate.shape[0]), bf16),
        VMEM((n_mp * rows, w_down.shape[1]), f32),
        VMEM((n, rows, width), bf16),
        VMEM((n, rows, width), bf16),
        pltpu.SemaphoreType.DMA((3,)),
    ]
    scratch += [pltpu.SemaphoreType.DMA((n,))] * 6
    scratch += [pltpu.SemaphoreType.DMA((len(bounds), 10))]
    for first, last in bounds:
        wide = last - first
        scratch += [
            VMEM((2, 2, rows, wide), f32),
            VMEM((2, 2, rows, wide), bf16),
            VMEM((2, 2, rows, wide), bf16),
            VMEM((2, rows, wide), bf16),
            VMEM((2, rows, wide), bf16),
            VMEM((n_mp, rows, wide), bf16),
        ]
    vmem, anywhere = pl.BlockSpec(memory_space=VMEM), pl.BlockSpec(memory_space=pl.ANY)
    return pl.pallas_call(
        functools.partial(ffn_kernel, plans, bounds),
        out_shape=jax.ShapeDtypeStruct((rows, width), bf16),
        in_specs=[vmem] * 3 + [anywhere] * 3,
        out_specs=vmem,
        scratch_shapes=scratch,
        compiler_params=pltpu.CompilerParams(
            collective_id=4, has_side_effects=True, vmem_limit_bytes=60 * 2**20
        ),
        name="ffn",
    )(scaled, square, residual, w_gate, w_up, w_down)


def joined(blocks):
    count, rows, width = blocks.shape
    return blocks.transpose(1, 0, 2).reshape(rows, count * width)


def body(
    n_seq,
    n_mp,
    tokens,
    gain_attn,
    w_query,
    query_bias,
    cache_keys,
    cache_values,
    w_out,
    gain_ffn,
    w_gate,
    w_up,
    w_down,
):
    seq, to_rows, home = (kind(n_seq, n_mp) for kind in (SeqPlan, RowsPlan, HomePlan))
    rows = tokens.shape[0]
    col_width = w_query.shape[1]
    offset = lax.axis_index("seq") * col_width
    hidden_in = tokens.astype(jnp.float32)
    mean_sq = jnp.mean(hidden_in * hidden_in, axis=1, keepdims=True)
    normed = (hidden_in * lax.rsqrt(mean_sq + eps) * gain_attn).astype(jnp.bfloat16)
    query_cols = (jnp.dot(normed, w_query, preferred_element_type=jnp.float32) + query_bias).astype(
        jnp.bfloat16
    )
    (query_blocks,) = exchange("queries", 1, (seq, query_cols, False))
    weighted, stats = attention(joined(query_blocks), cache_keys, cache_values)
    weighted = weighted.reshape(rows, n_seq, col_width).transpose(1, 0, 2)
    weighted, stats = exchange("merge", 2, (seq, weighted, True), (seq, stats, False))
    maxima, sums = stats[:, :, :HEADS], stats[:, :, SUM_LANE : SUM_LANE + HEADS]
    rescale = jnp.exp(maxima - jnp.max(maxima, axis=0, keepdims=True))
    totals = jnp.sum(sums * rescale, axis=0, keepdims=True)
    head_of = (offset + lax.broadcasted_iota(jnp.int32, (HEADS, col_width), 1)) // HEAD
    pick = (head_of == lax.broadcasted_iota(jnp.int32, (HEADS, col_width), 0)).astype(jnp.float32)
    factor = jnp.einsum(
        "jrh,hc->jrc", rescale / totals, pick, precision=lax.Precision.HIGHEST
    )
    attended = jnp.sum(weighted.astype(jnp.float32) * factor, axis=0).astype(jnp.bfloat16)
    (attended_blocks,) = exchange("attended", 3, (seq, attended, False))
    projected = jnp.dot(joined(attended_blocks), w_out, preferred_element_type=jnp.float32)
    residual = lax.dynamic_slice_in_dim(hidden_in, offset, col_width, 1) + projected
    square_part = jnp.sum(residual * residual, axis=1)[None, :]
    scaled = (residual * gain_ffn).astype(jnp.bfloat16)
    layer_out = ffn(
        (seq, to_rows, home), scaled, square_part, residual, w_gate, w_up, w_down
    )
    return (attended, layer_out)


def solution(mesh):
    placed = (
        P("mp", None),
        P(),
        P(None, "seq"),
        P("seq"),
        P(None, "seq", None),
        P(None, "seq", None),
        P(None, "seq"),
        P("seq"),
        P("mp", "seq"),
        P("mp", "seq"),
        P("seq", "mp"),
    )
    return jax.shard_map(
        functools.partial(body, mesh.shape["seq"], mesh.shape["mp"]),
        mesh=mesh,
        in_specs=placed,
        out_specs=(P("mp", "seq"), P("mp", "seq")),
        check_vma=False,
    )
```

```python
import functools

import jax
import jax.numpy as jnp
from jax import lax
from jax.experimental import pallas as pl
from jax.experimental.pallas import tpu as pltpu
from jax.sharding import PartitionSpec as P

D = 3584
HEADS = 28
KV_HEADS = 4
HEAD = 128
GROUP = HEADS // KV_HEADS
SUM_ROW = 8
CHUNKS = 4

eps = 1e-06
MESH = pl.DeviceIdType.MESH
VMEM = pltpu.VMEM


class SeqPlan:
    def __init__(self, n_seq, n_mp):
        self.count = n_seq

    def dest(self, s, m, i):
        to = lax.rem(s + i, self.count)
        return to, m, to

    def my_slot(self, s, m):
        return s

    def source(self, s, m, i):
        return i, m


class StatPlan(SeqPlan):
    def dest(self, s, m, i):
        to = lax.rem(s + i, self.count)
        return to, m, to // (self.count // KV_HEADS)


class RowsPlan:
    def __init__(self, n_seq, n_mp):
        self.count, self.per = n_seq, n_seq // n_mp

    def dest(self, s, m, i):
        to = lax.rem(s + i, self.count)
        return to, s // self.per, to

    def my_slot(self, s, m):
        return m * self.per + lax.rem(s, self.per)

    def source(self, s, m, i):
        return m * self.per + i % self.per, i // self.per


class HomePlan:
    def __init__(self, n_seq, n_mp):
        self.count, self.per, self.n_mp = n_seq, n_seq // n_mp, n_mp

    def dest(self, s, m, i):
        to_m = lax.rem(m + i // self.per, self.n_mp)
        j = lax.rem(s + i, self.per)
        return m * self.per + j, to_m, to_m * self.per + j

    def my_slot(self, s, m):
        return s

    def source(self, s, m, i):
        return i, s // self.per


def greet(plans, s, m):
    barrier = pltpu.get_barrier_semaphore()
    total = 0
    for plan in plans:
        for i in range(plan.count):
            pl.semaphore_signal(
                barrier, inc=1, device_id=plan.source(s, m, i), device_id_type=MESH
            )
        total += plan.count
    pl.semaphore_wait(barrier, total)


def push(src, dst, send, recv, to):
    return pltpu.make_async_remote_copy(
        src_ref=src,
        dst_ref=dst,
        send_sem=send,
        recv_sem=recv,
        device_id=to,
        device_id_type=MESH,
    )


class Flow:
    def __init__(self, plan, src, dst, spread, send, recv, s, m):
        self.plan, self.src, self.dst, self.spread = plan, src, dst, spread
        self.send, self.recv, self.s, self.m = send, recv, s, m
        self.started = []

    def start(self, i):
        to_s, to_m, index = self.plan.dest(self.s, self.m, i)
        mine = self.plan.my_slot(self.s, self.m)
        block = self.src.at[index] if self.spread else self.src
        here = jnp.logical_and(to_s == self.s, to_m == self.m)
        remote = push(block, self.dst.at[mine], self.send.at[i], self.recv.at[mine], (to_s, to_m))
        local = pltpu.make_async_copy(block, self.dst.at[mine], self.send.at[i])

        @pl.when(here)
        def _():
            local.start()

        @pl.when(jnp.logical_not(here))
        def _():
            remote.start()

        self.started.append((here, local, remote))

    def arrive(self):
        for i in range(self.plan.count):
            from_s, from_m = self.plan.source(self.s, self.m, i)
            block = self.src.at[0] if self.spread else self.src
            copy = push(block, self.dst.at[i], self.recv.at[i], self.recv.at[i], (from_s, from_m))

            @pl.when(jnp.logical_not(jnp.logical_and(from_s == self.s, from_m == self.m)))
            def _():
                copy.wait_recv()

        for here, local, remote in self.started:

            @pl.when(here)
            def _():
                local.wait()

    def left(self):
        for here, local, remote in self.started:

            @pl.when(jnp.logical_not(here))
            def _():
                remote.wait_send()


def exchange_kernel(plans, spread, *refs):
    k = len(plans)
    ins, outs, sems = refs[:k], refs[k : 2 * k], refs[2 * k :]
    s, m = lax.axis_index("seq"), lax.axis_index("mp")
    greet(list({type(plan): plan for plan in plans}.values()), s, m)
    flows = [
        Flow(plans[a], ins[a], outs[a], spread[a], sems[2 * a], sems[2 * a + 1], s, m)
        for a in range(k)
    ]
    for i in range(max(plan.count for plan in plans)):
        for flow in flows:
            if i < flow.plan.count:
                flow.start(i)
    for flow in flows:
        flow.arrive()
    for flow in flows:
        flow.left()


def exchange(name, cid, *items):
    plans = [item[0] for item in items]
    arrays = [item[1] for item in items]
    spread = [item[2] for item in items]
    shapes = []
    sems = []
    for plan, array, one_each in items:
        block = array.shape[1:] if one_each else array.shape
        shapes.append(jax.ShapeDtypeStruct((plan.count,) + block, array.dtype))
        sems += [pltpu.SemaphoreType.DMA((plan.count,))] * 2
    return pl.pallas_call(
        functools.partial(exchange_kernel, plans, spread),
        out_shape=tuple(shapes),
        in_specs=[pl.BlockSpec(memory_space=VMEM)] * len(items),
        out_specs=tuple([pl.BlockSpec(memory_space=VMEM)] * len(items)),
        scratch_shapes=sems,
        compiler_params=pltpu.CompilerParams(collective_id=cid, has_side_effects=True),
        name=name,
    )(*arrays)


def gather_kernel(n, src, out, sems):
    s, m = lax.axis_index("seq"), lax.axis_index("mp")
    half = n // 2
    hi, lo = s // 2, lax.rem(s, 2)
    partner = (hi * 2 + 1 - lo, m)
    barrier = pltpu.get_barrier_semaphore()
    peers = [lax.rem(hi + d, half) * 2 + lo for d in range(half)]
    for peer in peers[1:]:
        pl.semaphore_signal(barrier, inc=1, device_id=(peer, m), device_id_type=MESH)
    pl.semaphore_signal(barrier, inc=1, device_id=partner, device_id_type=MESH)
    pl.semaphore_wait(barrier, half)
    own = pltpu.make_async_copy(src, out.at[s], sems.at[4, 0])
    own.start()
    direct = [
        push(src, out.at[s], sems.at[0, d], sems.at[1, d], (peers[d], m)) for d in range(1, half)
    ]
    for copy in direct:
        copy.start()
    handed = [push(src, out.at[s], sems.at[2, 0], sems.at[3, 0], partner)]
    handed[0].start()
    for d in range(1, half):
        direct[d - 1].wait_recv()
        at = lax.rem(hi + half - d, half) * 2 + lo
        copy = push(out.at[at], out.at[at], sems.at[2, d], sems.at[3, d], partner)
        copy.start()
        handed.append(copy)
    for copy in handed:
        copy.wait_recv()
    own.wait()
    for copy in direct + handed:
        copy.wait_send()


def gather(name, cid, n, block):
    vmem = pl.BlockSpec(memory_space=VMEM)
    return pl.pallas_call(
        functools.partial(gather_kernel, n),
        out_shape=jax.ShapeDtypeStruct((n,) + block.shape, block.dtype),
        in_specs=[vmem],
        out_specs=vmem,
        scratch_shapes=[pltpu.SemaphoreType.DMA((5, n // 2))],
        compiler_params=pltpu.CompilerParams(collective_id=cid, has_side_effects=True),
        name=name,
    )(block)


def attention_kernel(q_ref, k_ref, v_ref, out_ref, stat_ref):
    count, rows, width = q_ref.shape
    q = jnp.concatenate([q_ref[j] for j in range(count)], axis=1)
    stacked = jnp.concatenate([q[:, h * HEAD : (h + 1) * HEAD] for h in range(GROUP)], axis=0)
    scores = times_transposed(stacked, k_ref[0]) * HEAD ** (-0.5)
    highest = jnp.max(scores, axis=1, keepdims=True)
    probs = jnp.exp(scores - highest)
    sums = jnp.sum(probs, axis=1, keepdims=True)
    weighted = jnp.dot(probs.astype(jnp.bfloat16), v_ref[0], preferred_element_type=jnp.float32)
    side = jnp.concatenate([weighted[h * rows : (h + 1) * rows] for h in range(GROUP)], axis=1)
    for j in range(count):
        out_ref[j] = side[:, j * width : (j + 1) * width].astype(jnp.bfloat16)
    stat_ref[...] = jnp.zeros_like(stat_ref)
    for h in range(GROUP):
        part = slice(h * rows, (h + 1) * rows)
        stat_ref[0, h : h + 1, :] = column_to_row(highest[part])
        stat_ref[0, h + SUM_ROW : h + SUM_ROW + 1, :] = column_to_row(sums[part])


def attention(queries, keys, values):
    n, rows, width = queries.shape
    context = keys.shape[1]
    count = n // KV_HEADS
    blocks = pl.BlockSpec((count, rows, width), lambda g: (g, 0, 0))
    cache = pl.BlockSpec((1, context, HEAD), lambda g: (g, 0, 0))
    return pl.pallas_call(
        attention_kernel,
        grid=(KV_HEADS,),
        out_shape=(
            jax.ShapeDtypeStruct((n, rows, width), jnp.bfloat16),
            jax.ShapeDtypeStruct((KV_HEADS, 2 * SUM_ROW, rows), jnp.float32),
        ),
        in_specs=[blocks, cache, cache],
        out_specs=(blocks, pl.BlockSpec((1, 2 * SUM_ROW, rows), lambda g: (g, 0, 0))),
        name="block_attention",
    )(queries, keys, values)


def merge_kernel(weighted_ref, stat_ref, out_ref):
    n, rows, width = weighted_ref.shape
    s = lax.axis_index("seq")
    maxima, sums = stat_ref[:, :SUM_ROW, :], stat_ref[:, SUM_ROW:, :]
    rescale = jnp.exp(maxima - jnp.max(maxima, axis=0, keepdims=True))
    total = jnp.sum(sums * rescale, axis=0)
    row = lax.broadcasted_iota(jnp.int32, (SUM_ROW, rows), 0)
    inverse = 1.0 / jnp.where(row < GROUP, total, 1.0)
    shape = (SUM_ROW, width)
    column = s * width + lax.broadcasted_iota(jnp.int32, shape, 1)
    head = lax.div(column, HEAD) - s // (n // KV_HEADS) * GROUP
    pick = jnp.where(head == lax.broadcasted_iota(jnp.int32, shape, 0), 1.0, 0.0)
    result = jnp.zeros((rows, width), jnp.float32)
    for j in range(n):
        factor = lax.dot_general(
            rescale[j] * inverse,
            pick,
            (((0,), (0,)), ((), ())),
            precision=lax.Precision.HIGHEST,
            preferred_element_type=jnp.float32,
        )
        result = result + weighted_ref[j].astype(jnp.float32) * factor
    out_ref[...] = result.astype(jnp.bfloat16)


def project_kernel(blocks, w_out, own_tokens, gain, residual, scaled, square):
    attended = jnp.concatenate([blocks[j] for j in range(blocks.shape[0])], axis=1)
    total = own_tokens[...] + times_transposed(attended, w_out[...])
    residual[...] = total
    scaled[...] = (total * gain[...]).astype(jnp.bfloat16)
    square[...] = column_to_row(jnp.sum(total * total, axis=1, keepdims=True))


def simple(kernel, out_shape, *arrays):
    return pl.pallas_call(kernel, out_shape=out_shape, name=kernel.__name__)(*arrays)


def times_transposed(a, b):
    return lax.dot_general(a, b, (((1,), (1,)), ((), ())), preferred_element_type=jnp.float32)


def row_to_column(row):
    k = row.shape[1]
    across = lax.broadcasted_iota(jnp.int32, (k, k), 1)
    down = lax.broadcasted_iota(jnp.int32, (k, k), 0)
    return jnp.sum(jnp.where(across == down, row, 0.0), axis=1, keepdims=True)


def column_to_row(column):
    k = column.shape[0]
    across = lax.broadcasted_iota(jnp.int32, (k, k), 1)
    down = lax.broadcasted_iota(jnp.int32, (k, k), 0)
    return jnp.sum(jnp.where(across == down, column, 0.0), axis=0, keepdims=True)


def ffn_kernel(plans, bounds, *refs):
    seq, to_rows, home = plans
    scaled, square, residual, gate_hbm, up_hbm, down_hbm, out = refs[:7]
    refs = refs[7:]
    gate_w, up_w, down_w, blocks, squares, features, acc, down_out, terms = refs[:9]
    refs = refs[9:]
    w_sems, sems = refs[0], refs[1:7]
    c_sems = refs[7]
    chunk_refs = refs[8:]
    s, m = lax.axis_index("seq"), lax.axis_index("mp")
    core, y = lax.rem(m, 2), m // 2
    sibling = (s, y * 2 + (1 - core))
    across = (s, (1 - y) * 2 + core)
    rows, width = scaled.shape
    per, n_mp = to_rows.per, home.n_mp
    loads = [
        pltpu.make_async_copy(gate_hbm, gate_w, w_sems.at[0]),
        pltpu.make_async_copy(up_hbm, up_w, w_sems.at[1]),
        pltpu.make_async_copy(down_hbm, down_w, w_sems.at[2]),
    ]
    for load in loads:
        load.start()
    barrier = pltpu.get_barrier_semaphore()
    for peer in (sibling, across):
        pl.semaphore_signal(barrier, inc=1, device_id=peer, device_id_type=MESH)
    for plan in plans:
        for i in range(plan.count):
            pl.semaphore_signal(
                barrier, inc=1, device_id=plan.source(s, m, i), device_id_type=MESH
            )
    pl.semaphore_wait(barrier, 2 + sum(plan.count for plan in plans))
    main = Flow(to_rows, scaled, blocks, False, sems[0], sems[1], s, m)
    side = Flow(seq, square, squares, False, sems[2], sems[3], s, m)
    for i in range(to_rows.count):
        main.start(i)
    for i in range(seq.count):
        side.start(i)
    main.arrive()
    order = (1 - core, 3 - core, core, 2 + core)
    for p, t in enumerate(order):
        features[p * rows : (p + 1) * rows, :] = jnp.concatenate(
            [blocks[t * per + j] for j in range(per)], axis=1
        )
    loads[0].wait()
    loads[1].wait()

    chunks = []
    for c, (first, last) in enumerate(bounds):
        kept, s1_out, s1_in, s2_out, s2_in, act = chunk_refs[6 * c : 6 * c + 6]
        sem = lambda k, c=c: c_sems.at[c, k]
        chunks.append(
            dict(
                first=first, last=last, kept=kept, s1_out=s1_out, s1_in=s1_in,
                s2_out=s2_out, s2_in=s2_in, act=act,
                s1=push(s1_out, s1_in, sem(0), sem(1), sibling),
                s2=push(s2_out, s2_in, sem(2), sem(3), across),
                near=push(act.at[m], act.at[m], sem(4), sem(5), sibling),
                far=push(act.at[m], act.at[m], sem(6), sem(7), across),
                relay=push(act.at[across[1]], act.at[across[1]], sem(8), sem(9), sibling),
            )
        )

    def multiply(ch):
        for g, weight in enumerate((gate_w, up_w)):
            part = times_transposed(features[...], weight[ch["first"] : ch["last"], :])
            for p in range(2):
                ch["s1_out"][g, p] = part[p * rows : (p + 1) * rows].astype(jnp.bfloat16)
                ch["kept"][g, p] = part[(p + 2) * rows : (p + 3) * rows]
        ch["s1"].start()

    def pair_sum(ch):
        ch["s1"].wait_recv()
        for g in range(2):
            ch["s2_out"][g] = (
                ch["kept"][g, 1 - y] + ch["s1_in"][g, 1 - y].astype(jnp.float32)
            ).astype(jnp.bfloat16)
        ch["s2"].start()

    def activate(ch, inverse):
        ch["s2"].wait_recv()
        total = [
            (
                ch["kept"][g, y]
                + ch["s1_in"][g, y].astype(jnp.float32)
                + ch["s2_in"][g].astype(jnp.float32)
            )
            * inverse
            for g in range(2)
        ]
        gate, up = total
        ch["act"][m] = (gate / (1.0 + jnp.exp(-gate)) * up).astype(jnp.bfloat16)
        ch["far"].start()
        ch["near"].start()

    for c, ch in enumerate(chunks):
        multiply(ch)
        if c >= 1:
            pair_sum(chunks[c - 1])
    pair_sum(chunks[-1])
    side.arrive()
    inverse = row_to_column(lax.rsqrt(jnp.sum(squares[...], axis=0) / D + eps))
    for ch in chunks:
        activate(ch, inverse)
    loads[2].wait()
    for c, ch in enumerate(chunks):
        ch["far"].wait_recv()
        ch["relay"].start()
        ch["near"].wait_recv()
        ch["relay"].wait_recv()
        act = ch["act"][...].reshape(n_mp * rows, ch["last"] - ch["first"])
        part = jnp.dot(
            act, down_w[ch["first"] : ch["last"], :], preferred_element_type=jnp.float32
        )
        if c < len(chunks) - 1:
            acc[...] = part if c == 0 else acc[...] + part
        else:
            total = part if c == 0 else acc[...] + part
            for t in range(n_mp):
                for j in range(per):
                    down_out[t * per + j] = total[
                        t * rows : (t + 1) * rows, j * width : (j + 1) * width
                    ].astype(jnp.bfloat16)
    last = Flow(home, down_out, terms, True, sems[4], sems[5], s, m)
    for i in range(home.count):
        last.start(i)
    last.arrive()
    result = residual[...]
    for i in range(home.count):
        result = result + terms[i].astype(jnp.float32)
    out[...] = result.astype(jnp.bfloat16)
    main.left()
    side.left()
    last.left()
    for ch in chunks:
        for name in ("s1", "s2", "near", "far", "relay"):
            ch[name].wait_send()


def ffn(plans, scaled, square, residual, w_gate, w_up, w_down):
    seq, to_rows, home = plans
    rows, width = scaled.shape
    n_mp, n = home.n_mp, home.count
    hidden = w_gate.shape[0]
    step = max(128, -(-hidden // CHUNKS // 128) * 128)
    bounds = [(at, min(at + step, hidden)) for at in range(0, hidden, step)]
    bf16, f32 = jnp.bfloat16, jnp.float32
    scratch = [
        VMEM(w_gate.shape, bf16),
        VMEM(w_up.shape, bf16),
        VMEM(w_down.shape, bf16),
        VMEM((n, rows, width), bf16),
        VMEM((n, 1, rows), f32),
        VMEM((n_mp * rows, w_gate.shape[1]), bf16),
        VMEM((n_mp * rows, w_down.shape[1]), f32),
        VMEM((n, rows, width), bf16),
        VMEM((n, rows, width), bf16),
        pltpu.SemaphoreType.DMA((3,)),
    ]
    scratch += [pltpu.SemaphoreType.DMA((n,))] * 6
    scratch += [pltpu.SemaphoreType.DMA((len(bounds), 10))]
    for first, last in bounds:
        wide = last - first
        scratch += [
            VMEM((2, 2, rows, wide), f32),
            VMEM((2, 2, rows, wide), bf16),
            VMEM((2, 2, rows, wide), bf16),
            VMEM((2, rows, wide), bf16),
            VMEM((2, rows, wide), bf16),
            VMEM((n_mp, rows, wide), bf16),
        ]
    vmem, anywhere = pl.BlockSpec(memory_space=VMEM), pl.BlockSpec(memory_space=pl.ANY)
    return pl.pallas_call(
        functools.partial(ffn_kernel, plans, bounds),
        out_shape=jax.ShapeDtypeStruct((rows, width), bf16),
        in_specs=[vmem] * 3 + [anywhere] * 3,
        out_specs=vmem,
        scratch_shapes=scratch,
        compiler_params=pltpu.CompilerParams(
            collective_id=4, has_side_effects=True, vmem_limit_bytes=60 * 2**20
        ),
        name="ffn",
    )(scaled, square, residual, w_gate, w_up, w_down)


def body(
    n_seq,
    n_mp,
    tokens,
    gain_attn,
    w_query,
    query_bias,
    cache_keys,
    cache_values,
    w_out,
    gain_ffn,
    w_gate,
    w_up,
    w_down,
):
    seq, to_rows, home = (kind(n_seq, n_mp) for kind in (SeqPlan, RowsPlan, HomePlan))
    rows = tokens.shape[0]
    col_width = w_query.shape[1]
    offset = lax.axis_index("seq") * col_width
    hidden_in = tokens.astype(jnp.float32)
    mean_sq = jnp.mean(hidden_in * hidden_in, axis=1, keepdims=True)
    normed = (hidden_in * lax.rsqrt(mean_sq + eps) * gain_attn).astype(jnp.bfloat16)
    query_cols = (jnp.dot(normed, w_query, preferred_element_type=jnp.float32) + query_bias).astype(
        jnp.bfloat16
    )
    query_blocks = gather("queries", 1, n_seq, query_cols)
    weighted, stats = attention(query_blocks, cache_keys, cache_values)
    weighted, stats = exchange(
        "merge", 2, (seq, weighted, True), (StatPlan(n_seq, n_mp), stats, True)
    )
    block = jax.ShapeDtypeStruct((rows, col_width), jnp.bfloat16)
    wide = jax.ShapeDtypeStruct((rows, col_width), jnp.float32)
    attended = simple(merge_kernel, block, weighted, stats)
    attended_blocks = gather("attended", 3, n_seq, attended)
    residual, scaled, square_part = simple(
        project_kernel,
        (wide, block, jax.ShapeDtypeStruct((1, rows), jnp.float32)),
        attended_blocks,
        w_out.T,
        lax.dynamic_slice_in_dim(hidden_in, offset, col_width, 1),
        gain_ffn[None, :],
    )
    layer_out = ffn(
        (seq, to_rows, home), scaled, square_part, residual, w_gate.T, w_up.T, w_down
    )
    return (attended, layer_out)


def solution(mesh):
    placed = (
        P("mp", None),
        P(),
        P(None, "seq"),
        P("seq"),
        P(None, "seq", None),
        P(None, "seq", None),
        P(None, "seq"),
        P("seq"),
        P("mp", "seq"),
        P("mp", "seq"),
        P("seq", "mp"),
    )
    return jax.shard_map(
        functools.partial(body, mesh.shape["seq"], mesh.shape["mp"]),
        mesh=mesh,
        in_specs=placed,
        out_specs=(P("mp", "seq"), P("mp", "seq")),
        check_vma=False,
    )
```

```python
import functools

import jax
import jax.numpy as jnp
from jax import lax
from jax.experimental import pallas as pl
from jax.experimental.pallas import tpu as pltpu
from jax.sharding import PartitionSpec as P

D = 3584
HEADS = 28
KV_HEADS = 4
HEAD = 128
GROUP = HEADS // KV_HEADS
SUM_ROW = 8
CHUNKS = 2
HALVES = 2

eps = 1e-06
MESH = pl.DeviceIdType.MESH
VMEM = pltpu.VMEM


class SeqPlan:
    def __init__(self, n_seq, n_mp):
        self.count = n_seq

    def dest(self, s, m, i):
        to = lax.rem(s + i, self.count)
        return to, m, to

    def my_slot(self, s, m):
        return s

    def source(self, s, m, i):
        return i, m


class StatPlan(SeqPlan):
    def dest(self, s, m, i):
        to = lax.rem(s + i, self.count)
        return to, m, to // (self.count // KV_HEADS)


class RowsPlan:
    def __init__(self, n_seq, n_mp):
        self.count, self.per = n_seq, n_seq // n_mp

    def dest(self, s, m, i):
        to = lax.rem(s + i, self.count)
        return to, s // self.per, to

    def my_slot(self, s, m):
        return m * self.per + lax.rem(s, self.per)

    def source(self, s, m, i):
        return m * self.per + i % self.per, i // self.per


class HomePlan:
    def __init__(self, n_seq, n_mp):
        self.count, self.per, self.n_mp = n_seq, n_seq // n_mp, n_mp

    def dest(self, s, m, i):
        to_m = lax.rem(m + i // self.per, self.n_mp)
        j = lax.rem(s + i, self.per)
        return m * self.per + j, to_m, to_m * self.per + j

    def my_slot(self, s, m):
        return s

    def source(self, s, m, i):
        return i, s // self.per


def greet(plans, s, m):
    barrier = pltpu.get_barrier_semaphore()
    total = 0
    for plan in plans:
        for i in range(plan.count):
            pl.semaphore_signal(
                barrier, inc=1, device_id=plan.source(s, m, i), device_id_type=MESH
            )
        total += plan.count
    pl.semaphore_wait(barrier, total)


def push(src, dst, send, recv, to):
    return pltpu.make_async_remote_copy(
        src_ref=src,
        dst_ref=dst,
        send_sem=send,
        recv_sem=recv,
        device_id=to,
        device_id_type=MESH,
    )


class Flow:
    def __init__(self, plan, src, dst, spread, send, recv, s, m):
        self.plan, self.src, self.dst, self.spread = plan, src, dst, spread
        self.send, self.recv, self.s, self.m = send, recv, s, m
        self.started = []

    def start(self, i):
        to_s, to_m, index = self.plan.dest(self.s, self.m, i)
        mine = self.plan.my_slot(self.s, self.m)
        block = self.src.at[index] if self.spread else self.src
        here = jnp.logical_and(to_s == self.s, to_m == self.m)
        remote = push(block, self.dst.at[mine], self.send.at[i], self.recv.at[mine], (to_s, to_m))
        local = pltpu.make_async_copy(block, self.dst.at[mine], self.send.at[i])

        @pl.when(here)
        def _():
            local.start()

        @pl.when(jnp.logical_not(here))
        def _():
            remote.start()

        self.started.append((here, local, remote))

    def arrive(self):
        for i in range(self.plan.count):
            from_s, from_m = self.plan.source(self.s, self.m, i)
            block = self.src.at[0] if self.spread else self.src
            copy = push(block, self.dst.at[i], self.recv.at[i], self.recv.at[i], (from_s, from_m))

            @pl.when(jnp.logical_not(jnp.logical_and(from_s == self.s, from_m == self.m)))
            def _():
                copy.wait_recv()

        for here, local, remote in self.started:

            @pl.when(here)
            def _():
                local.wait()

    def left(self):
        for here, local, remote in self.started:

            @pl.when(jnp.logical_not(here))
            def _():
                remote.wait_send()


def exchange_kernel(plans, spread, *refs):
    k = len(plans)
    ins, outs, sems = refs[:k], refs[k : 2 * k], refs[2 * k :]
    s, m = lax.axis_index("seq"), lax.axis_index("mp")
    greet(list({type(plan): plan for plan in plans}.values()), s, m)
    flows = [
        Flow(plans[a], ins[a], outs[a], spread[a], sems[2 * a], sems[2 * a + 1], s, m)
        for a in range(k)
    ]
    for i in range(max(plan.count for plan in plans)):
        for flow in flows:
            if i < flow.plan.count:
                flow.start(i)
    for flow in flows:
        flow.arrive()
    for flow in flows:
        flow.left()


def exchange(name, cid, *items):
    plans = [item[0] for item in items]
    arrays = [item[1] for item in items]
    spread = [item[2] for item in items]
    shapes = []
    sems = []
    for plan, array, one_each in items:
        block = array.shape[1:] if one_each else array.shape
        shapes.append(jax.ShapeDtypeStruct((plan.count,) + block, array.dtype))
        sems += [pltpu.SemaphoreType.DMA((plan.count,))] * 2
    return pl.pallas_call(
        functools.partial(exchange_kernel, plans, spread),
        out_shape=tuple(shapes),
        in_specs=[pl.BlockSpec(memory_space=VMEM)] * len(items),
        out_specs=tuple([pl.BlockSpec(memory_space=VMEM)] * len(items)),
        scratch_shapes=sems,
        compiler_params=pltpu.CompilerParams(collective_id=cid, has_side_effects=True),
        name=name,
    )(*arrays)


def gather_kernel(n, src, out, sems):
    s, m = lax.axis_index("seq"), lax.axis_index("mp")
    half = n // 2
    hi, lo = s // 2, lax.rem(s, 2)
    partner = (hi * 2 + 1 - lo, m)
    barrier = pltpu.get_barrier_semaphore()
    peers = [lax.rem(hi + d, half) * 2 + lo for d in range(half)]
    for peer in peers[1:]:
        pl.semaphore_signal(barrier, inc=1, device_id=(peer, m), device_id_type=MESH)
    pl.semaphore_signal(barrier, inc=1, device_id=partner, device_id_type=MESH)
    pl.semaphore_wait(barrier, half)
    own = pltpu.make_async_copy(src, out.at[s], sems.at[4, 0])
    own.start()
    direct = [
        push(src, out.at[s], sems.at[0, d], sems.at[1, d], (peers[d], m)) for d in range(1, half)
    ]
    for copy in direct:
        copy.start()
    handed = [push(src, out.at[s], sems.at[2, 0], sems.at[3, 0], partner)]
    handed[0].start()
    for d in range(1, half):
        direct[d - 1].wait_recv()
        at = lax.rem(hi + half - d, half) * 2 + lo
        copy = push(out.at[at], out.at[at], sems.at[2, d], sems.at[3, d], partner)
        copy.start()
        handed.append(copy)
    for copy in handed:
        copy.wait_recv()
    own.wait()
    for copy in direct + handed:
        copy.wait_send()


def gather(name, cid, n, block):
    vmem = pl.BlockSpec(memory_space=VMEM)
    return pl.pallas_call(
        functools.partial(gather_kernel, n),
        out_shape=jax.ShapeDtypeStruct((n,) + block.shape, block.dtype),
        in_specs=[vmem],
        out_specs=vmem,
        scratch_shapes=[pltpu.SemaphoreType.DMA((5, n // 2))],
        compiler_params=pltpu.CompilerParams(collective_id=cid, has_side_effects=True),
        name=name,
    )(block)


def attention_kernel(q_ref, k_ref, v_ref, out_ref, stat_ref):
    count, rows, width = q_ref.shape
    q = jnp.concatenate([q_ref[j] for j in range(count)], axis=1)
    stacked = jnp.concatenate([q[:, h * HEAD : (h + 1) * HEAD] for h in range(GROUP)], axis=0)
    scores = times_transposed(stacked, k_ref[0]) * HEAD ** (-0.5)
    highest = jnp.max(scores, axis=1, keepdims=True)
    probs = jnp.exp(scores - highest)
    sums = jnp.sum(probs, axis=1, keepdims=True)
    weighted = jnp.dot(probs.astype(jnp.bfloat16), v_ref[0], preferred_element_type=jnp.float32)
    side = jnp.concatenate([weighted[h * rows : (h + 1) * rows] for h in range(GROUP)], axis=1)
    for j in range(count):
        out_ref[j] = side[:, j * width : (j + 1) * width].astype(jnp.bfloat16)
    stat_ref[...] = jnp.zeros_like(stat_ref)
    for h in range(GROUP):
        part = slice(h * rows, (h + 1) * rows)
        stat_ref[0, h : h + 1, :] = column_to_row(highest[part])
        stat_ref[0, h + SUM_ROW : h + SUM_ROW + 1, :] = column_to_row(sums[part])


def attention(queries, keys, values):
    n, rows, width = queries.shape
    context = keys.shape[1]
    count = n // KV_HEADS
    blocks = pl.BlockSpec((count, rows, width), lambda g: (g, 0, 0))
    cache = pl.BlockSpec((1, context, HEAD), lambda g: (g, 0, 0))
    return pl.pallas_call(
        attention_kernel,
        grid=(KV_HEADS,),
        out_shape=(
            jax.ShapeDtypeStruct((n, rows, width), jnp.bfloat16),
            jax.ShapeDtypeStruct((KV_HEADS, 2 * SUM_ROW, rows), jnp.float32),
        ),
        in_specs=[blocks, cache, cache],
        out_specs=(blocks, pl.BlockSpec((1, 2 * SUM_ROW, rows), lambda g: (g, 0, 0))),
        name="block_attention",
    )(queries, keys, values)


def merge_kernel(weighted_ref, stat_ref, out_ref):
    n, rows, width = weighted_ref.shape
    s = lax.axis_index("seq")
    maxima, sums = stat_ref[:, :SUM_ROW, :], stat_ref[:, SUM_ROW:, :]
    rescale = jnp.exp(maxima - jnp.max(maxima, axis=0, keepdims=True))
    total = jnp.sum(sums * rescale, axis=0)
    row = lax.broadcasted_iota(jnp.int32, (SUM_ROW, rows), 0)
    inverse = 1.0 / jnp.where(row < GROUP, total, 1.0)
    shape = (SUM_ROW, width)
    column = s * width + lax.broadcasted_iota(jnp.int32, shape, 1)
    head = lax.div(column, HEAD) - s // (n // KV_HEADS) * GROUP
    pick = jnp.where(head == lax.broadcasted_iota(jnp.int32, shape, 0), 1.0, 0.0)
    result = jnp.zeros((rows, width), jnp.float32)
    for j in range(n):
        factor = lax.dot_general(
            rescale[j] * inverse,
            pick,
            (((0,), (0,)), ((), ())),
            precision=lax.Precision.HIGHEST,
            preferred_element_type=jnp.float32,
        )
        result = result + weighted_ref[j].astype(jnp.float32) * factor
    out_ref[...] = result.astype(jnp.bfloat16)


def project_kernel(blocks, w_out, own_tokens, gain, residual, scaled, square):
    attended = jnp.concatenate([blocks[j] for j in range(blocks.shape[0])], axis=1)
    total = own_tokens[...] + times_transposed(attended, w_out[...])
    residual[...] = total
    scaled[...] = (total * gain[...]).astype(jnp.bfloat16)
    square[...] = column_to_row(jnp.sum(total * total, axis=1, keepdims=True))


def simple(kernel, out_shape, *arrays):
    return pl.pallas_call(kernel, out_shape=out_shape, name=kernel.__name__)(*arrays)


def times_transposed(a, b):
    return lax.dot_general(a, b, (((1,), (1,)), ((), ())), preferred_element_type=jnp.float32)


def row_to_column(row):
    k = row.shape[1]
    across = lax.broadcasted_iota(jnp.int32, (k, k), 1)
    down = lax.broadcasted_iota(jnp.int32, (k, k), 0)
    return jnp.sum(jnp.where(across == down, row, 0.0), axis=1, keepdims=True)


def column_to_row(column):
    k = column.shape[0]
    across = lax.broadcasted_iota(jnp.int32, (k, k), 1)
    down = lax.broadcasted_iota(jnp.int32, (k, k), 0)
    return jnp.sum(jnp.where(across == down, column, 0.0), axis=0, keepdims=True)


def ffn_kernel(plans, bounds, *refs):
    seq, to_rows, home = plans
    scaled, square, residual, gate_hbm, up_hbm, down_hbm, out = refs[:7]
    refs = refs[7:]
    gate_w, up_w, down_w, blocks, squares, features, acc, down_out, terms = refs[:9]
    refs = refs[9:]
    w_sems, sems = refs[0], refs[1 : 3 + 4 * HALVES]
    c_sems = refs[3 + 4 * HALVES]
    chunk_refs = refs[4 + 4 * HALVES :]
    s, m = lax.axis_index("seq"), lax.axis_index("mp")
    core, y = lax.rem(m, 2), m // 2
    sibling = (s, y * 2 + (1 - core))
    across = (s, (1 - y) * 2 + core)
    rows, width = scaled.shape[0] // HALVES, scaled.shape[1]
    per, n_mp = to_rows.per, home.n_mp
    loads = [
        pltpu.make_async_copy(gate_hbm, gate_w, w_sems.at[0]),
        pltpu.make_async_copy(up_hbm, up_w, w_sems.at[1]),
        pltpu.make_async_copy(down_hbm, down_w, w_sems.at[2]),
    ]
    for load in loads:
        load.start()
    barrier = pltpu.get_barrier_semaphore()
    for peer in (sibling, across):
        pl.semaphore_signal(barrier, inc=1, device_id=peer, device_id_type=MESH)
    for plan in plans:
        for i in range(plan.count):
            pl.semaphore_signal(
                barrier, inc=1, device_id=plan.source(s, m, i), device_id_type=MESH
            )
    pl.semaphore_wait(barrier, 2 + sum(plan.count for plan in plans))
    mains = [
        Flow(
            to_rows, scaled.at[pl.ds(h * rows, rows)], blocks.at[h], False,
            sems[2 + 4 * h], sems[3 + 4 * h], s, m,
        )
        for h in range(HALVES)
    ]
    side = Flow(seq, square, squares, False, sems[0], sems[1], s, m)
    for main in mains:
        for i in range(to_rows.count):
            main.start(i)
    for i in range(seq.count):
        side.start(i)
    order = (1 - core, 3 - core, core, 2 + core)

    def collect(h):
        mains[h].arrive()
        for p, t in enumerate(order):
            features[h, p * rows : (p + 1) * rows, :] = jnp.concatenate(
                [blocks[h, t * per + j] for j in range(per)], axis=1
            )

    chunks = []
    for c, (h, first, last) in enumerate(bounds):
        kept, s1_out, s1_in, s2_out, s2_in, act = chunk_refs[6 * c : 6 * c + 6]
        sem = lambda k, c=c: c_sems.at[c, k]
        chunks.append(
            dict(
                half=h, first=first, last=last, kept=kept, s1_out=s1_out, s1_in=s1_in,
                s2_out=s2_out, s2_in=s2_in, act=act,
                s1=push(s1_out, s1_in, sem(0), sem(1), sibling),
                s2=push(s2_out, s2_in, sem(2), sem(3), across),
                near=push(act.at[m], act.at[m], sem(4), sem(5), sibling),
                far=push(act.at[m], act.at[m], sem(6), sem(7), across),
                relay=push(act.at[across[1]], act.at[across[1]], sem(8), sem(9), sibling),
            )
        )

    def multiply(ch):
        for g, weight in enumerate((gate_w, up_w)):
            part = times_transposed(features[ch["half"]], weight[ch["first"] : ch["last"], :])
            for p in range(2):
                ch["s1_out"][g, p] = part[p * rows : (p + 1) * rows].astype(jnp.bfloat16)
                ch["kept"][g, p] = part[(p + 2) * rows : (p + 3) * rows]
        ch["s1"].start()

    def pair_sum(ch):
        ch["s1"].wait_recv()
        for g in range(2):
            ch["s2_out"][g] = (
                ch["kept"][g, 1 - y] + ch["s1_in"][g, 1 - y].astype(jnp.float32)
            ).astype(jnp.bfloat16)
        ch["s2"].start()

    def activate(ch, inverse):
        ch["s2"].wait_recv()
        total = [
            (
                ch["kept"][g, y]
                + ch["s1_in"][g, y].astype(jnp.float32)
                + ch["s2_in"][g].astype(jnp.float32)
            )
            * inverse
            for g in range(2)
        ]
        gate, up = total
        ch["act"][m] = (gate / (1.0 + jnp.exp(-gate)) * up).astype(jnp.bfloat16)
        ch["far"].start()
        ch["near"].start()

    def finish(h):
        own = halves[h]
        for c, ch in enumerate(own):
            ch["far"].wait_recv()
            ch["relay"].start()
            ch["near"].wait_recv()
            ch["relay"].wait_recv()
            act = ch["act"][...].reshape(n_mp * rows, ch["last"] - ch["first"])
            part = jnp.dot(
                act, down_w[ch["first"] : ch["last"], :], preferred_element_type=jnp.float32
            )
            total = part if c == 0 else acc[...] + part
            if c < len(own) - 1:
                acc[...] = total
        for t in range(n_mp):
            for j in range(per):
                down_out[h, t * per + j] = total[
                    t * rows : (t + 1) * rows, j * width : (j + 1) * width
                ].astype(jnp.bfloat16)
        flow = Flow(
            home, down_out.at[h], terms.at[h], True, sems[4 + 4 * h], sems[5 + 4 * h], s, m
        )
        for i in range(home.count):
            flow.start(i)
        return flow

    halves = [[ch for ch in chunks if ch["half"] == h] for h in range(HALVES)]
    collect(0)
    loads[0].wait()
    loads[1].wait()
    for c, ch in enumerate(halves[0]):
        multiply(ch)
        if c >= 1:
            pair_sum(halves[0][c - 1])
    pair_sum(halves[0][-1])
    side.arrive()
    inverse = row_to_column(lax.rsqrt(jnp.sum(squares[...], axis=0) / D + eps))
    finals = []
    for h in range(1, HALVES):
        collect(h)
        for ch in halves[h]:
            multiply(ch)
        for ch in halves[h - 1]:
            activate(ch, inverse[(h - 1) * rows : h * rows])
        for ch in halves[h]:
            pair_sum(ch)
        if h == 1:
            loads[2].wait()
        finals.append(finish(h - 1))
    for ch in halves[-1]:
        activate(ch, inverse[(HALVES - 1) * rows : HALVES * rows])
    finals.append(finish(HALVES - 1))
    for h, flow in enumerate(finals):
        flow.arrive()
        part = slice(h * rows, (h + 1) * rows)
        result = residual[part, :]
        for i in range(home.count):
            result = result + terms[h, i].astype(jnp.float32)
        out[part, :] = result.astype(jnp.bfloat16)
    for flow in mains + [side] + finals:
        flow.left()
    for ch in chunks:
        for name in ("s1", "s2", "near", "far", "relay"):
            ch[name].wait_send()


def ffn(plans, scaled, square, residual, w_gate, w_up, w_down):
    seq, to_rows, home = plans
    rows, width = scaled.shape
    n_mp, n = home.n_mp, home.count
    hidden = w_gate.shape[0]
    step = max(128, -(-hidden // CHUNKS // 128) * 128)
    bounds = [
        (h, at, min(at + step, hidden))
        for h in range(HALVES)
        for at in range(0, hidden, step)
    ]
    part = rows // HALVES
    bf16, f32 = jnp.bfloat16, jnp.float32
    scratch = [
        VMEM(w_gate.shape, bf16),
        VMEM(w_up.shape, bf16),
        VMEM(w_down.shape, bf16),
        VMEM((HALVES, n, part, width), bf16),
        VMEM((n, 1, rows), f32),
        VMEM((HALVES, n_mp * part, w_gate.shape[1]), bf16),
        VMEM((n_mp * part, w_down.shape[1]), f32),
        VMEM((HALVES, n, part, width), bf16),
        VMEM((HALVES, n, part, width), bf16),
        pltpu.SemaphoreType.DMA((3,)),
    ]
    scratch += [pltpu.SemaphoreType.DMA((n,))] * (2 + 4 * HALVES)
    scratch += [pltpu.SemaphoreType.DMA((len(bounds), 10))]
    for _, first, last in bounds:
        wide = last - first
        scratch += [
            VMEM((2, 2, part, wide), f32),
            VMEM((2, 2, part, wide), bf16),
            VMEM((2, 2, part, wide), bf16),
            VMEM((2, part, wide), bf16),
            VMEM((2, part, wide), bf16),
            VMEM((n_mp, part, wide), bf16),
        ]
    vmem, anywhere = pl.BlockSpec(memory_space=VMEM), pl.BlockSpec(memory_space=pl.ANY)
    return pl.pallas_call(
        functools.partial(ffn_kernel, plans, bounds),
        out_shape=jax.ShapeDtypeStruct((rows, width), bf16),
        in_specs=[vmem] * 3 + [anywhere] * 3,
        out_specs=vmem,
        scratch_shapes=scratch,
        compiler_params=pltpu.CompilerParams(
            collective_id=4, has_side_effects=True, vmem_limit_bytes=60 * 2**20
        ),
        name="ffn",
    )(scaled, square, residual, w_gate, w_up, w_down)


def body(
    n_seq,
    n_mp,
    tokens,
    gain_attn,
    w_query,
    query_bias,
    cache_keys,
    cache_values,
    w_out,
    gain_ffn,
    w_gate,
    w_up,
    w_down,
):
    seq, to_rows, home = (kind(n_seq, n_mp) for kind in (SeqPlan, RowsPlan, HomePlan))
    rows = tokens.shape[0]
    col_width = w_query.shape[1]
    offset = lax.axis_index("seq") * col_width
    hidden_in = tokens.astype(jnp.float32)
    mean_sq = jnp.mean(hidden_in * hidden_in, axis=1, keepdims=True)
    normed = (hidden_in * lax.rsqrt(mean_sq + eps) * gain_attn).astype(jnp.bfloat16)
    query_cols = (jnp.dot(normed, w_query, preferred_element_type=jnp.float32) + query_bias).astype(
        jnp.bfloat16
    )
    query_blocks = gather("queries", 1, n_seq, query_cols)
    weighted, stats = attention(query_blocks, cache_keys, cache_values)
    weighted, stats = exchange(
        "merge", 2, (seq, weighted, True), (StatPlan(n_seq, n_mp), stats, True)
    )
    block = jax.ShapeDtypeStruct((rows, col_width), jnp.bfloat16)
    wide = jax.ShapeDtypeStruct((rows, col_width), jnp.float32)
    attended = simple(merge_kernel, block, weighted, stats)
    attended_blocks = gather("attended", 3, n_seq, attended)
    residual, scaled, square_part = simple(
        project_kernel,
        (wide, block, jax.ShapeDtypeStruct((1, rows), jnp.float32)),
        attended_blocks,
        w_out.T,
        lax.dynamic_slice_in_dim(hidden_in, offset, col_width, 1),
        gain_ffn[None, :],
    )
    layer_out = ffn(
        (seq, to_rows, home), scaled, square_part, residual, w_gate.T, w_up.T, w_down
    )
    return (attended, layer_out)


def solution(mesh):
    placed = (
        P("mp", None),
        P(),
        P(None, "seq"),
        P("seq"),
        P(None, "seq", None),
        P(None, "seq", None),
        P(None, "seq"),
        P("seq"),
        P("mp", "seq"),
        P("mp", "seq"),
        P("seq", "mp"),
    )
    return jax.shard_map(
        functools.partial(body, mesh.shape["seq"], mesh.shape["mp"]),
        mesh=mesh,
        in_specs=placed,
        out_specs=(P("mp", "seq"), P("mp", "seq")),
        check_vma=False,
    )
```
